32 devices in a mesh: grp: 2 (over y), slab: 4 (over z), ang: 4 (over x, core).
Axes of the slice: x: 2, y: 2, z: 4, core: 2. Of those that a mesh axis runs over, the one named last changes fastest.
Arguments:
- volume: bfloat16 [16, 256, 1024], P(('grp', 'slab')), parts along dimension 0, may hold values from -6 to 6
- ray_weights: bfloat16 [8, 1024, 1024], P('ang'), may hold values from -0.0625 to 0.0625
- row_offsets: int32 [8, 8], P('ang'), may hold values from 0 to 8
- measured: float32 [16, 256, 1024], P(('grp', 'ang'), 'slab'), parts along dimension 0, may hold values from -6 to 6
- shifts: float32 [16], P(('grp', 'ang')), parts along dimension 0, may hold values from -4 to 4
Outputs:
- updated_volume: bfloat16 [16, 256, 1024], P(('grp', 'slab')), parts along dimension 0
- last_residual: float32 [16, 256, 1024], P(('grp', 'ang'), 'slab'), parts along dimension 0
- shift_slope: float32 [16], P(('grp', 'ang')), parts along dimension 0
The draws below stay inside these ranges and needn't reach their ends.
There are 2 independent parts, one for each index of `grp`. The reference program is written for one: setup_inputs(seed, part) draws one part's arguments, and reference() takes and returns one part's arrays. A program takes and returns all parts, laid end to end along the dimension named above; an argument that names none is the same for every part. Nothing has to cross between parts.
All inputs are finite; a program needn't handle non-finite values.
Results may differ from the reference program's by a relative error of at most 0.006.
Values may be sent and summed in bfloat16 or wider, within the bound.
A program may use at most 128 MiB of HBM per device.

```python
import math
import jax
import jax.numpy as jnp
from jax import lax

ANG_DEV = 2
Y = 256
X = 1024
U = 1024
OFF = 8
ROUNDS = 2
NZ = 8
ANGLES = 8
N_ANG = 4


def touch_ends(entries, stream_key, least, high):
    extent = entries.shape
    index_at = [jax.random.randint(jax.random.fold_in(stream_key, axis), (), 0, extent[axis]) for axis in range(len(extent))]
    entries = entries.at[tuple(index_at)].set(least)
    longest = extent.index(max(extent))
    index_at[longest] = (index_at[longest] + 1) % extent[longest]
    return entries.at[tuple(index_at)].set(high)


def level_of(key, dims, split, smallest, largest):
    factor_of = 1.0
    for axis_at, parts in split:
        draws = jax.random.uniform(jax.random.fold_in(jax.random.fold_in(key, 6), axis_at), (parts,), jnp.float32, smallest / len(split), largest / len(split))
        factor_of = factor_of * jnp.repeat(jnp.exp(draws), dims[axis_at] // parts).reshape((-1,) + (1,) * (len(dims) - 1 - axis_at))
    return factor_of


def scatter_about(stream_key, dims, scale, limit, shards=(), dtype=jnp.bfloat16):
    result = scale * jax.random.normal(stream_key, dims, jnp.float32)
    if shards:
        result = result * level_of(stream_key, dims, shards, -0.22, 0.18)
    return jnp.clip(result, -limit, limit).astype(dtype)


def setup_inputs(seed: int = 0, part: int = 0) -> dict:
    splits = jax.random.split(jax.random.key(seed), 6)
    part_splits = jax.random.split(jax.random.fold_in(splits[5], part), 6)
    volume = scatter_about(part_splits[0], (NZ, Y, X), 1.0, 6.0, ((0, 4),))
    ray_weights = scatter_about(splits[1], (ANGLES, X, U), (X * NZ) ** -0.5, 0.0625, ((0, 4),))
    row_offsets = touch_ends(jax.random.randint(splits[2], (ANGLES, NZ), 0, OFF + 1), jax.random.fold_in(splits[2], 1), 0, OFF).astype(jnp.int32)
    measured = scatter_about(part_splits[3], (ANGLES, Y, U), 1.0, 6.0, ((0, 4), (1, 4)), jnp.float32)
    shifts = jnp.clip(jax.random.uniform(part_splits[4], (ANGLES,), jnp.float32, -4.0, 4.0) * level_of(part_splits[4], (ANGLES,), ((0, 4),), -0.4, 0.0), -4.0, 4.0)
    return dict(volume=volume, ray_weights=ray_weights, row_offsets=row_offsets, measured=measured, shifts=shifts)


step_size = 0.5

def move_down(products, tilt_table):
    base = jnp.zeros((Y + OFF, U), jnp.float32)
    placed = jax.vmap(lambda block, shift_rows: lax.dynamic_update_slice(base, block, (shift_rows, jnp.int32(0))))(products, tilt_table)
    return lax.optimization_barrier(jnp.sum(placed, axis=0))[:Y]

def reference(volume, ray_weights, row_offsets, measured, shifts):
    frequency = jnp.fft.fftfreq(U).astype(jnp.float32)
    spectrum = jnp.fft.fft(measured.astype(jnp.float32), axis=-1)
    phase = jnp.exp(-2j * jnp.pi * frequency[None, :] * shifts[:, None])
    rotated = spectrum * phase[:, None, :]
    shifted = jnp.real(jnp.fft.ifft(rotated, axis=-1)).astype(jnp.float32)
    slope_field = jnp.real(jnp.fft.ifft(rotated * (-2j * jnp.pi * frequency)[None, None, :], axis=-1)).astype(jnp.float32)
    current = volume
    projection = shifted
    residual = shifted
    for round_index in range(ROUNDS):
        flattened = current.astype(jnp.float32).reshape(NZ * Y, X)
        projection = jnp.stack([move_down(jnp.dot(flattened, ray_weights[angle_index].astype(jnp.float32), preferred_element_type=jnp.float32).reshape(NZ, Y, U), row_offsets[angle_index]) for angle_index in range(ANGLES)])
        residual = projection - shifted
        rounded = residual.astype(jnp.bfloat16)
        padded = jnp.concatenate([rounded, jnp.zeros((ANGLES, OFF, U), jnp.bfloat16)], axis=1)
        gradient = jnp.zeros((NZ * Y, X), jnp.float32)
        for group_index in range(N_ANG):
            running = jnp.zeros((NZ * Y, X), jnp.float32)
            for angle_index in range(group_index * ANG_DEV, (group_index + 1) * ANG_DEV):
                source = padded[angle_index]
                picked = jax.vmap(lambda shift_rows: lax.dynamic_slice(source, (shift_rows, jnp.int32(0)), (Y, U)))(row_offsets[angle_index])
                running = running + jnp.dot(picked.reshape(NZ * Y, U).astype(jnp.float32), ray_weights[angle_index].astype(jnp.float32).T, preferred_element_type=jnp.float32)
            partial_value = lax.optimization_barrier(running.astype(jnp.bfloat16))
            gradient = gradient + partial_value.astype(jnp.float32)
        current = (current.astype(jnp.float32) - step_size * gradient.reshape(NZ, Y, X)).astype(jnp.bfloat16)
    shift_slope = lax.optimization_barrier(jnp.sum(projection * slope_field, axis=(1, 2))) / math.sqrt(Y * U)
    return (current, residual, shift_slope)
```

```python
import math

import functools

import jax
import jax.numpy as jnp
import numpy as np
from jax import lax
from jax.experimental import pallas as pl
from jax.experimental.pallas import tpu as pltpu
from jax.sharding import PartitionSpec as P

Y = 256
X = 1024
U = 1024
OFF = 8
ROUNDS = 2


step_size = 0.5


def move_down(products, tilt_table):
    base = jnp.zeros((products.shape[1] + OFF, U), jnp.float32)
    placed = jax.vmap(
        lambda block, shift_rows: lax.dynamic_update_slice(base, block, (shift_rows, jnp.int32(0)))
    )(products, tilt_table)
    return jnp.sum(placed, axis=0)


def backproject(extended, tilt_table, ray_weights, band_rows):
    slices_count = tilt_table.shape[1]
    running = jnp.zeros((slices_count * band_rows, X), jnp.float32)
    for angle_index in range(ray_weights.shape[0]):
        source = extended[angle_index]
        picked = jax.vmap(
            lambda shift_rows: lax.dynamic_slice(source, (shift_rows, jnp.int32(0)), (band_rows, U))
        )(tilt_table[angle_index])
        running = running + lax.dot_general(
            picked.reshape(slices_count * band_rows, U),
            ray_weights[angle_index],
            (((1,), (1,)), ((), ())),
            preferred_element_type=jnp.float32,
        )
    return running


def apply_update(current, running):
    partial_value = lax.optimization_barrier(running.reshape(current.shape).astype(jnp.bfloat16))
    partial_wide = partial_value.astype(jnp.float32)
    gradient = lax.psum(partial_wide, "ang")
    renewed = (current.astype(jnp.float32) - step_size * gradient).astype(jnp.bfloat16)
    return renewed


def per_device(volume, ray_weights, row_offsets, measured, shifts):
    angles_here = ray_weights.shape[0]
    band_rows = measured.shape[1]
    highest = lax.Precision.HIGHEST
    numbers = lax.iota(jnp.int32, U)
    turns = numbers[:, None] * numbers[None, :] % U
    radians = turns.astype(jnp.float32) * (2.0 * math.pi / U)
    cosine = jnp.cos(radians)
    sine = jnp.sin(radians)
    signed = jnp.where(numbers <= (U - 1) // 2, numbers, numbers - U)
    omega = signed.astype(jnp.float32) * (2.0 * math.pi / U)
    flat_rows = measured.reshape(angles_here * band_rows, U)
    real_part = jnp.dot(flat_rows, cosine, precision=highest).reshape(angles_here, band_rows, U)
    imag_part = -jnp.dot(flat_rows, sine, precision=highest).reshape(angles_here, band_rows, U)
    phase = omega[None, None, :] * shifts[:, None, None]
    turned_real = real_part * jnp.cos(phase) + imag_part * jnp.sin(phase)
    turned_imag = imag_part * jnp.cos(phase) - real_part * jnp.sin(phase)
    first_half = jnp.concatenate([turned_real, omega * turned_imag], axis=0).reshape(-1, U)
    second_half = jnp.concatenate([turned_imag, -omega * turned_real], axis=0).reshape(-1, U)
    inverse = (
        jnp.dot(first_half, cosine, precision=highest)
        - jnp.dot(second_half, sine, precision=highest)
    ) / U
    inverse = inverse.reshape(2, angles_here, band_rows, U)
    shifted = inverse[0]
    slope_field = inverse[1]
    projection = shifted
    residual = shifted
    current = volume
    slices_here = volume.shape[0]
    tilt_table = lax.dynamic_slice_in_dim(
        row_offsets, lax.axis_index("slab") * slices_here, slices_here, 1
    )
    for round_index in range(ROUNDS):
        flattened = current.reshape(slices_here * Y, X)
        partials = jnp.stack(
            [
                move_down(
                    jnp.dot(
                        flattened, ray_weights[angle_index], preferred_element_type=jnp.float32
                    ).reshape(slices_here, Y, U),
                    tilt_table[angle_index],
                )[:Y]
                for angle_index in range(angles_here)
            ]
        )
        projection = lax.psum_scatter(partials, "slab", scatter_dimension=1, tiled=True)
        residual = projection - shifted
        rounded = residual.astype(jnp.bfloat16)
        gathered = lax.all_gather(rounded, "slab", axis=1, tiled=True)
        extended = jnp.concatenate(
            [gathered, jnp.zeros((angles_here, OFF, U), jnp.bfloat16)], axis=1
        )
        running = backproject(extended, tilt_table, ray_weights, Y)
        current = apply_update(current, running)
    local_dot = jnp.sum(projection * slope_field, axis=(1, 2))
    shift_slope = lax.psum(local_dot, "slab") / math.sqrt(Y * U)
    return (current, residual, shift_slope)


F32 = jnp.float32
BF16 = jnp.bfloat16
HALO = 16
FINE = 32


def wave_tables(columns):
    half = columns // 2
    k = np.arange(half)[None, :]
    coarse = np.arange(columns // FINE)[:, None] * FINE
    fine = np.arange(FINE)[:, None]
    turn = 2.0 * np.pi / columns
    coarse_turns = (coarse * k % columns) * turn
    fine_turns = (fine * k % columns) * turn
    fine_sine = np.sin(fine_turns)
    fine_sine[:, 0] = 1.0 - 2.0 * (np.arange(FINE) % 2)
    tables = (np.cos(coarse_turns), np.sin(coarse_turns), np.cos(fine_turns), fine_sine)
    return [jnp.asarray(t.astype(np.float32)) for t in tables]


def split(value):
    high = value.astype(BF16)
    return high, (value - high.astype(F32)).astype(BF16)


def dot(a, b):
    return jnp.dot(a, b, preferred_element_type=F32)


def dot_t(a, b):
    return lax.dot_general(a, b, (((1,), (1,)), ((), ())), preferred_element_type=F32)


def fit_kernel(
    n, m, off, shifts, vol, w_hbm, meas, ctab, stab, ftab, gtab,
    out, res_out, slope_out,
    w, wave_hi, wave_lo, spec, wide, field, db, dh, ub, band, halo, acc, ext,
    psend, precv, own, xsend, xrecv, fresh, sl,
    w_sem, loc_sem, zs, zr, ags, agr, rhs, rhr, ps, pr, xs, xr, hs, hr, fs, fr, os_, or_, ss, sr,
):
    slab = lax.axis_index("slab")
    me = lax.axis_index("ang")
    angles, rows, cols = meas.shape
    slices = vol.shape[0]
    nz = slices * n
    qc = vol.shape[2] // m
    mate = me + 1 - 2 * (me % 2)
    across = (me + 2) % m
    diagonal = (mate + 2) % m
    later = (slab + 1) % n
    earlier = (slab + n - 1) % n

    def remote(src, dst, send, recv, **where):
        return pltpu.make_async_remote_copy(
            src_ref=src, dst_ref=dst, send_sem=send, recv_sem=recv,
            device_id=where, device_id_type=pl.DeviceIdType.MESH,
        )

    w_copy = pltpu.make_async_copy(w_hbm, w, w_sem)
    w_copy.start()
    barrier = pltpu.get_barrier_semaphore()
    for hop in range(1, n):
        pl.semaphore_signal(
            barrier, 1, device_id={"slab": (slab + hop) % n}, device_id_type=pl.DeviceIdType.MESH
        )
    for peer in (mate, across):
        pl.semaphore_signal(barrier, 1, device_id={"ang": peer}, device_id_type=pl.DeviceIdType.MESH)
    pl.semaphore_wait(barrier, n + 1)

    def quarter(q):
        return pl.ds(pl.multiple_of(q * qc, qc), qc)

    def band_rows(d):
        return pl.ds(pl.multiple_of(d * rows, rows), rows)

    def halo_rows(d):
        return pl.ds(pl.multiple_of((d + n - 1) % n * rows + rows - HALO, HALO), HALO)

    mine = pl.ds(slab * slices, slices)
    first = []
    for hop in range(1, n):
        d = (slab + hop) % n
        first.append(remote(vol.at[:, band_rows(d), quarter(me)], band.at[0, me, mine],
                            zs.at[hop - 1], zr.at[hop - 1], slab=d))
        first.append(remote(vol.at[:, halo_rows(d), quarter(me)], halo.at[0, me, mine],
                            zs.at[n - 2 + hop], zr.at[n - 2 + hop], slab=d))
    for copy in first:
        copy.start()
    local = [
        pltpu.make_async_copy(vol.at[:, band_rows(slab), quarter(me)], band.at[0, me, mine], loc_sem.at[0]),
        pltpu.make_async_copy(vol.at[:, halo_rows(slab), quarter(me)], halo.at[0, me, mine], loc_sem.at[1]),
    ]
    for copy in local:
        copy.start()

    half = cols // 2

    def wave_rows(i, carry):
        at = pl.ds(pl.multiple_of(i * FINE, FINE), FINE)
        cc, cs = ctab[pl.ds(i, 1), :], stab[pl.ds(i, 1), :]
        fc, fs_ = ftab[...], gtab[...]
        hi, lo = split(cc * fc - cs * fs_)
        wave_hi[at, :half] = hi
        wave_lo[at, :half] = lo
        hi, lo = split(cs * fc + cc * fs_)
        wave_hi[at, half:] = hi
        wave_lo[at, half:] = lo
        return carry

    lax.fori_loop(0, cols // FINE, wave_rows, 0)
    flat = angles * rows
    x_hi, x_lo = split(meas[...].reshape(flat, cols))
    wide[:flat, :] = x_hi
    wide[flat : 2 * flat, :] = x_lo
    tile = 256

    def forward(j, carry):
        at = pl.ds(pl.multiple_of(j * tile, tile), tile)
        both = dot(wide[: 2 * flat, :], wave_hi[:, at])
        spec[:, at] = both[:flat] + both[flat:] + dot(wide[:flat, :], wave_lo[:, at])
        return carry

    lax.fori_loop(0, cols // tile, forward, 0)

    def gather_start(t, kind, buf, q):
        return [
            remote(buf.at[t, q], buf.at[t, q], ags.at[t, kind, 0], agr.at[t, kind, 0], ang=across),
            remote(buf.at[t, q], buf.at[t, q], ags.at[t, kind, 1], agr.at[t, kind, 1], ang=mate),
            remote(buf.at[t, across], buf.at[t, across], ags.at[t, kind, 2], agr.at[t, kind, 2], ang=mate),
        ]

    for copy in first:
        copy.wait()
    for copy in local:
        copy.wait()
    gathers = [gather_start(0, 0, band, me), gather_start(0, 1, halo, me)]
    for gather in gathers:
        gather[0].start()
        gather[1].start()

    column = lax.broadcasted_iota(jnp.int32, (1, half), 1)
    base = column == 0
    omega = column.astype(F32) * (2.0 * math.pi / cols)
    turn_rate = jnp.where(base, math.pi, omega)
    weight = jnp.where(base, 1.0 / cols, 2.0 / cols)
    for a in range(angles):
        phase = turn_rate * shifts[a]
        cn, sn = jnp.cos(phase), jnp.sin(phase)
        cr = jnp.where(base, 1.0, cn)
        sr_ = jnp.where(base, 0.0, sn)
        re = spec[a * rows : (a + 1) * rows, :half]
        im = spec[a * rows : (a + 1) * rows, half:]
        parts = (
            (re * cr - im * sr_) * weight,
            (im * cn + re * sr_) * weight,
            (im * cr + re * sr_) * (-omega * weight),
            re * (omega * weight * cr) - im * (turn_rate * weight * sn),
        )
        for which in range(2):
            at = (which * angles + a) * rows
            for side in range(2):
                hi, lo = split(parts[2 * which + side])
                wide[at : at + rows, side * half : (side + 1) * half] = hi
                wide[2 * flat + at : 2 * flat + at + rows, side * half : (side + 1) * half] = lo

    def backward(j, carry):
        at = pl.ds(pl.multiple_of(j * tile, tile), tile)
        both = dot_t(wide[...], wave_hi[at, :])
        field[:, at] = both[: 2 * flat] + both[2 * flat :] + dot_t(wide[: 2 * flat, :], wave_lo[at, :])
        return carry

    lax.fori_loop(0, cols // tile, backward, 0)

    for depth, target in ((rows, db), (HALO, dh)):
        row = lax.broadcasted_iota(jnp.int32, (rows, nz * depth), 0)
        col = lax.broadcasted_iota(jnp.int32, (rows, nz * depth), 1)
        for a in range(angles):
            moved = row - col % depth
            for z in range(nz):
                moved = jnp.where(col // depth == z, moved - off[a, z], moved)
            if target is dh:
                moved = moved + HALO
                hit = jnp.where(moved == 0, jnp.where(slab > 0, 1.0, 0.0), 0.0)
            else:
                hit = jnp.where(moved == 0, 1.0, 0.0)
            target[a * rows : (a + 1) * rows, :] = hit.astype(BF16)

    tall_rows = rows + HALO
    row = lax.broadcasted_iota(jnp.int32, (rows, 2 * angles * tall_rows), 0)
    col = lax.broadcasted_iota(jnp.int32, (rows, 2 * angles * tall_rows), 1)
    for z in range(nz):
        moved = col % tall_rows - row
        for a in range(angles):
            moved = jnp.where(col // tall_rows % angles == a, moved - off[a, z], moved)
        ub[z * rows : (z + 1) * rows, :] = jnp.where(moved == 0, 1.0, 0.0).astype(BF16)

    w_copy.wait()

    def project(t, q, fresh_sum):
        moved = dot(db[...], band[t, q].reshape(nz * rows, qc)) + dot(dh[...], halo[t, q].reshape(nz * HALO, qc))
        hi, lo = split(moved)
        for a in range(angles):
            both = jnp.concatenate([hi[a * rows : (a + 1) * rows], lo[a * rows : (a + 1) * rows]], axis=0)
            part = dot(both, w[a, quarter(q), :])
            acc[a] = part if fresh_sum else acc[a] + part

    def spread(q, store):
        backs = [split(dot_t(ext_now[a], w[a, quarter(q), :])) for a in range(angles)]
        tall = jnp.concatenate([hi for hi, _ in backs] + [lo for _, lo in backs], axis=0)
        store(dot(ub[...], tall).astype(BF16).reshape(nz, rows, qc))

    pending = []
    for t in range(ROUNDS):
        last = t == ROUNDS - 1
        project(t, me, True) if t == 0 else None
        if t > 0:
            halo_copy.wait()
            gathers.append(gather_start(t, 1, halo, me))
            gathers[1][0].start()
            gathers[1][1].start()
            project(t, me, True)
        for gather in gathers:
            gather[0].wait_recv()
            gather[2].start()
        project(t, across, False)
        for gather in gathers:
            gather[1].wait_recv()
        project(t, mate, False)
        for gather in gathers:
            gather[2].wait_recv()
        project(t, diagonal, False)
        for gather in gathers:
            pending.extend(gather)
        ext_now = ext.at[t]
        for a in range(angles):
            projection = acc[a, :rows, :] + acc[a, rows:, :]
            residual = projection - field[a * rows : (a + 1) * rows, :]
            ext_now[a, :rows, :] = residual.astype(BF16)
            if last:
                res_out[a] = residual
                slope = field[(angles + a) * rows : (angles + a + 1) * rows, :]
                line = jnp.sum(projection * slope, axis=0, keepdims=True)
                sl[0, pl.ds(a, 1), :] = line
        edge = remote(ext_now.at[:, :HALO, :], ext_now.at[:, pl.ds(rows, HALO), :], rhs.at[t], rhr.at[t], slab=earlier)
        edge.start()
        if last:
            slopes = []
            for hop in range(1, n):
                slopes.append(remote(sl.at[0], sl.at[hop], ss.at[hop - 1], sr.at[hop - 1], slab=(slab + hop) % n))
                slopes[-1].start()
        edge.wait()
        keep = jnp.where(slab < n - 1, 1.0, 0.0)
        for a in range(angles):
            ext_now[a, rows:, :] = (ext_now[a, rows:, :].astype(F32) * keep).astype(BF16)

        sends = []
        for slot, q in ((0, diagonal), (1, mate)):
            def put(value, slot=slot):
                psend[t, slot] = value
            spread(q, put)
            copy = remote(psend.at[t, slot], precv.at[t, slot], ps.at[t, slot], pr.at[t, slot], ang=mate)
            copy.start()
            sends.append(copy)

        def put_own(value):
            own[...] = value

        spread(across, put_own)
        sends[0].wait_recv()
        xsend[t] = (own[...].astype(F32) + precv[t, 0].astype(F32)).astype(BF16)
        x_copy = remote(xsend.at[t], xrecv.at[t], xs.at[t], xr.at[t], ang=across)
        x_copy.start()
        spread(me, put_own)
        sends[1].wait_recv()
        x_copy.wait_recv()
        pending.extend(sends)
        pending.append(x_copy)
        gradient = own[...].astype(F32) + precv[t, 1].astype(F32) + xrecv[t].astype(F32)
        renewed = (band[t, me].astype(F32) - step_size * gradient).astype(BF16)
        if last:
            fresh[...] = renewed
        else:
            band[t + 1, me] = renewed
            halo_copy = remote(
                band.at[t + 1, me, :, pl.ds(rows - HALO, HALO), :], halo.at[t + 1, me], hs.at[t], hr.at[t], slab=later
            )
            halo_copy.start()
            gathers = [gather_start(t + 1, 0, band, me)]
            gathers[0][0].start()
            gathers[0][1].start()

    finals = []
    for hop in range(1, n):
        d = (slab + hop) % n
        finals.append(remote(fresh.at[pl.ds(d * slices, slices)], out.at[:, band_rows(slab), quarter(me)],
                             fs.at[hop - 1], fr.at[hop - 1], slab=d))
        finals[-1].start()
    keep_own = pltpu.make_async_copy(fresh.at[mine], out.at[:, band_rows(slab), quarter(me)], loc_sem.at[2])
    keep_own.start()
    for copy in slopes:
        copy.wait_recv()
    total = sl[0]
    for hop in range(1, n):
        total = total + sl[hop]
    slope_out[...] = jnp.broadcast_to(
        jnp.sum(total, axis=1, keepdims=True) * (1.0 / math.sqrt(rows * n * cols)), slope_out.shape
    )
    for copy in finals:
        copy.wait_recv()
    keep_own.wait()
    mine_out = out.at[:, :, quarter(me)]
    across_out = out.at[:, :, quarter(across)]
    ends = [
        remote(mine_out, mine_out, os_.at[0], or_.at[0], ang=across),
        remote(mine_out, mine_out, os_.at[1], or_.at[1], ang=mate),
        remote(across_out, across_out, os_.at[2], or_.at[2], ang=mate),
    ]
    ends[0].start()
    ends[1].start()
    ends[0].wait_recv()
    ends[2].start()
    ends[1].wait_recv()
    ends[2].wait_recv()
    for copy in pending + slopes + finals + ends:
        copy.wait_send()


def fused(n, m, volume, ray_weights, row_offsets, measured, shifts):
    angles, rows, cols = measured.shape
    slices, _, xcells = volume.shape
    nz = slices * n
    qc = xcells // m
    flat = angles * rows
    quad = (nz, rows, qc)
    dma = pltpu.SemaphoreType.DMA
    vmem = pl.BlockSpec(memory_space=pltpu.VMEM)
    smem = pl.BlockSpec(memory_space=pltpu.SMEM)
    current, residual, slope = pl.pallas_call(
        functools.partial(fit_kernel, n, m),
        name="fit",
        out_shape=(
            jax.ShapeDtypeStruct(volume.shape, BF16),
            jax.ShapeDtypeStruct(measured.shape, F32),
            jax.ShapeDtypeStruct((angles, 128), F32),
        ),
        in_specs=[smem, smem, vmem, pl.BlockSpec(memory_space=pl.ANY), vmem] + [vmem] * 4,
        out_specs=(vmem, vmem, vmem),
        scratch_shapes=[
            pltpu.VMEM(ray_weights.shape, BF16),
            pltpu.VMEM((cols, cols), BF16),
            pltpu.VMEM((cols, cols), BF16),
            pltpu.VMEM((flat, cols), F32),
            pltpu.VMEM((4 * flat, cols), BF16),
            pltpu.VMEM((2 * flat, cols), F32),
            pltpu.VMEM((flat, nz * rows), BF16),
            pltpu.VMEM((flat, nz * HALO), BF16),
            pltpu.VMEM((nz * rows, 2 * angles * (rows + HALO)), BF16),
            pltpu.VMEM((ROUNDS, m) + quad, BF16),
            pltpu.VMEM((ROUNDS, m, nz, HALO, qc), BF16),
            pltpu.VMEM((angles, 2 * rows, cols), F32),
            pltpu.VMEM((ROUNDS, angles, rows + HALO, cols), BF16),
            pltpu.VMEM((ROUNDS, 2) + quad, BF16),
            pltpu.VMEM((ROUNDS, 2) + quad, BF16),
            pltpu.VMEM(quad, BF16),
            pltpu.VMEM((ROUNDS,) + quad, BF16),
            pltpu.VMEM((ROUNDS,) + quad, BF16),
            pltpu.VMEM(quad, BF16),
            pltpu.VMEM((n, angles, cols), F32),
            dma, dma((3,)),
            dma((2 * n - 2,)), dma((2 * n - 2,)),
            dma((ROUNDS, 2, 3)), dma((ROUNDS, 2, 3)),
            dma((ROUNDS,)), dma((ROUNDS,)),
            dma((ROUNDS, 2)), dma((ROUNDS, 2)),
            dma((ROUNDS,)), dma((ROUNDS,)),
            dma((ROUNDS,)), dma((ROUNDS,)),
            dma((n - 1,)), dma((n - 1,)),
            dma((3,)), dma((3,)),
            dma((n - 1,)), dma((n - 1,)),
        ],
        compiler_params=pltpu.CompilerParams(
            collective_id=0, has_side_effects=True, vmem_limit_bytes=60 * 1024 * 1024
        ),
    )(row_offsets, shifts, volume, ray_weights, measured, *wave_tables(cols))
    return current, residual, slope[:, 0]


def step(n, m, volume, ray_weights, row_offsets, measured, shifts):
    band_rows = measured.shape[1]
    if m == 4 and n > 1 and band_rows % HALO == 0 and OFF <= HALO:
        return fused(n, m, volume, ray_weights, row_offsets, measured, shifts)
    return per_device(volume, ray_weights, row_offsets, measured, shifts)


def solution(mesh):
    local = functools.partial(step, mesh.shape["slab"], mesh.shape["ang"])
    in_specs = (
        P(("grp", "slab"), None, None),
        P("ang", None, None),
        P("ang", None),
        P(("grp", "ang"), "slab", None),
        P(("grp", "ang")),
    )
    out_specs = (P(("grp", "slab"), None, None), P(("grp", "ang"), "slab", None), P(("grp", "ang")))
    return jax.shard_map(
        local, mesh=mesh, in_specs=in_specs, out_specs=out_specs, check_vma=False
    )
```

```python
import math

import functools

import jax
import jax.numpy as jnp
import numpy as np
from jax import lax
from jax.experimental import pallas as pl
from jax.experimental.pallas import tpu as pltpu
from jax.sharding import PartitionSpec as P

Y = 256
X = 1024
U = 1024
OFF = 8
ROUNDS = 2


step_size = 0.5


def move_down(products, tilt_table):
    base = jnp.zeros((products.shape[1] + OFF, U), jnp.float32)
    placed = jax.vmap(
        lambda block, shift_rows: lax.dynamic_update_slice(base, block, (shift_rows, jnp.int32(0)))
    )(products, tilt_table)
    return jnp.sum(placed, axis=0)


def backproject(extended, tilt_table, ray_weights, band_rows):
    slices_count = tilt_table.shape[1]
    running = jnp.zeros((slices_count * band_rows, X), jnp.float32)
    for angle_index in range(ray_weights.shape[0]):
        source = extended[angle_index]
        picked = jax.vmap(
            lambda shift_rows: lax.dynamic_slice(source, (shift_rows, jnp.int32(0)), (band_rows, U))
        )(tilt_table[angle_index])
        running = running + lax.dot_general(
            picked.reshape(slices_count * band_rows, U),
            ray_weights[angle_index],
            (((1,), (1,)), ((), ())),
            preferred_element_type=jnp.float32,
        )
    return running


def apply_update(current, running):
    partial_value = lax.optimization_barrier(running.reshape(current.shape).astype(jnp.bfloat16))
    partial_wide = partial_value.astype(jnp.float32)
    gradient = lax.psum(partial_wide, "ang")
    renewed = (current.astype(jnp.float32) - step_size * gradient).astype(jnp.bfloat16)
    return renewed


def per_device(volume, ray_weights, row_offsets, measured, shifts):
    angles_here = ray_weights.shape[0]
    band_rows = measured.shape[1]
    highest = lax.Precision.HIGHEST
    numbers = lax.iota(jnp.int32, U)
    turns = numbers[:, None] * numbers[None, :] % U
    radians = turns.astype(jnp.float32) * (2.0 * math.pi / U)
    cosine = jnp.cos(radians)
    sine = jnp.sin(radians)
    signed = jnp.where(numbers <= (U - 1) // 2, numbers, numbers - U)
    omega = signed.astype(jnp.float32) * (2.0 * math.pi / U)
    flat_rows = measured.reshape(angles_here * band_rows, U)
    real_part = jnp.dot(flat_rows, cosine, precision=highest).reshape(angles_here, band_rows, U)
    imag_part = -jnp.dot(flat_rows, sine, precision=highest).reshape(angles_here, band_rows, U)
    phase = omega[None, None, :] * shifts[:, None, None]
    turned_real = real_part * jnp.cos(phase) + imag_part * jnp.sin(phase)
    turned_imag = imag_part * jnp.cos(phase) - real_part * jnp.sin(phase)
    first_half = jnp.concatenate([turned_real, omega * turned_imag], axis=0).reshape(-1, U)
    second_half = jnp.concatenate([turned_imag, -omega * turned_real], axis=0).reshape(-1, U)
    inverse = (
        jnp.dot(first_half, cosine, precision=highest)
        - jnp.dot(second_half, sine, precision=highest)
    ) / U
    inverse = inverse.reshape(2, angles_here, band_rows, U)
    shifted = inverse[0]
    slope_field = inverse[1]
    projection = shifted
    residual = shifted
    current = volume
    slices_here = volume.shape[0]
    tilt_table = lax.dynamic_slice_in_dim(
        row_offsets, lax.axis_index("slab") * slices_here, slices_here, 1
    )
    for round_index in range(ROUNDS):
        flattened = current.reshape(slices_here * Y, X)
        partials = jnp.stack(
            [
                move_down(
                    jnp.dot(
                        flattened, ray_weights[angle_index], preferred_element_type=jnp.float32
                    ).reshape(slices_here, Y, U),
                    tilt_table[angle_index],
                )[:Y]
                for angle_index in range(angles_here)
            ]
        )
        projection = lax.psum_scatter(partials, "slab", scatter_dimension=1, tiled=True)
        residual = projection - shifted
        rounded = residual.astype(jnp.bfloat16)
        gathered = lax.all_gather(rounded, "slab", axis=1, tiled=True)
        extended = jnp.concatenate(
            [gathered, jnp.zeros((angles_here, OFF, U), jnp.bfloat16)], axis=1
        )
        running = backproject(extended, tilt_table, ray_weights, Y)
        current = apply_update(current, running)
    local_dot = jnp.sum(projection * slope_field, axis=(1, 2))
    shift_slope = lax.psum(local_dot, "slab") / math.sqrt(Y * U)
    return (current, residual, shift_slope)


F32 = jnp.float32
BF16 = jnp.bfloat16
HALO = 16
FINE = 32


def wave_tables(columns):
    half = columns // 2
    k = np.arange(half)[None, :]
    coarse = np.arange(columns // FINE)[:, None] * FINE
    fine = np.arange(FINE)[:, None]
    turn = 2.0 * np.pi / columns
    coarse_turns = (coarse * k % columns) * turn
    fine_turns = (fine * k % columns) * turn
    fine_sine = np.sin(fine_turns)
    fine_sine[:, 0] = 1.0 - 2.0 * (np.arange(FINE) % 2)
    tables = (np.cos(coarse_turns), np.sin(coarse_turns), np.cos(fine_turns), fine_sine)
    return [jnp.asarray(t.astype(np.float32)) for t in tables]


def split(value):
    high = value.astype(BF16)
    return high, (value - high.astype(F32)).astype(BF16)


def dot(a, b):
    return jnp.dot(a, b, preferred_element_type=F32)


def dot_t(a, b):
    return lax.dot_general(a, b, (((1,), (1,)), ((), ())), preferred_element_type=F32)


def fit_kernel(
    n, m, off, shifts, vol, w_hbm, meas, ctab, stab, ftab, gtab,
    out, res_out, slope_out,
    w, wave_hi, wave_lo, spec, wide, field, db, dh, ub, band, halo, acc, ext,
    psend, precv, own, xsend, xrecv, fresh, sl,
    w_sem, loc_sem, zs, zr, gs, gr, ags, agr, rhs, rhr, ps, pr, xs, xr, cs, cr_, hs, hr, fs, fr, os_, or_, ss, sr,
):
    slab = lax.axis_index("slab")
    me = lax.axis_index("ang")
    angles, rows, cols = meas.shape
    slices = vol.shape[0]
    nz = slices * n
    qc = vol.shape[2] // m
    mate = me + 1 - 2 * (me % 2)
    across = (me + 2) % m
    diagonal = (mate + 2) % m
    later = (slab + 1) % n
    earlier = (slab + n - 1) % n

    def remote(src, dst, send, recv, **where):
        return pltpu.make_async_remote_copy(
            src_ref=src, dst_ref=dst, send_sem=send, recv_sem=recv,
            device_id=where, device_id_type=pl.DeviceIdType.MESH,
        )

    w_copy = pltpu.make_async_copy(w_hbm, w, w_sem)
    w_copy.start()
    barrier = pltpu.get_barrier_semaphore()
    for hop in range(1, n):
        pl.semaphore_signal(
            barrier, 1, device_id={"slab": (slab + hop) % n}, device_id_type=pl.DeviceIdType.MESH
        )
    for peer in (mate, across):
        pl.semaphore_signal(barrier, 1, device_id={"ang": peer}, device_id_type=pl.DeviceIdType.MESH)
    pl.semaphore_wait(barrier, n + 1)

    def quarter(q):
        return pl.ds(pl.multiple_of(q * qc, qc), qc)

    def band_rows(d):
        return pl.ds(pl.multiple_of(d * rows, rows), rows)

    def halo_rows(d):
        return pl.ds(pl.multiple_of((d + n - 1) % n * rows + rows - HALO, HALO), HALO)

    mine = pl.ds(slab * slices, slices)
    first = []
    for hop in range(1, n):
        d = (slab + hop) % n
        first.append(remote(vol.at[:, band_rows(d), quarter(me)], band.at[0, me, mine],
                            zs.at[hop - 1], zr.at[hop - 1], slab=d))
        first.append(remote(vol.at[:, halo_rows(d), quarter(me)], halo.at[0, me, mine],
                            zs.at[n - 2 + hop], zr.at[n - 2 + hop], slab=d))
    for copy in first:
        copy.start()
    local = []
    for q in range(m):
        columns = pl.ds(q * qc, qc)
        local.append(pltpu.make_async_copy(vol.at[:, band_rows(slab), columns], band.at[0, q, mine], loc_sem.at[2 * q]))
        local.append(pltpu.make_async_copy(vol.at[:, halo_rows(slab), columns], halo.at[0, q, mine], loc_sem.at[2 * q + 1]))
    for copy in local:
        copy.start()

    half = cols // 2

    def wave_rows(i, carry):
        at = pl.ds(pl.multiple_of(i * FINE, FINE), FINE)
        cc, cs = ctab[pl.ds(i, 1), :], stab[pl.ds(i, 1), :]
        fc, fs_ = ftab[...], gtab[...]
        hi, lo = split(cc * fc - cs * fs_)
        wave_hi[at, :half] = hi
        wave_lo[at, :half] = lo
        hi, lo = split(cs * fc + cc * fs_)
        wave_hi[at, half:] = hi
        wave_lo[at, half:] = lo
        return carry

    lax.fori_loop(0, cols // FINE, wave_rows, 0)
    flat = angles * rows
    x_hi, x_lo = split(meas[...].reshape(flat, cols))
    wide[:flat, :] = x_hi
    wide[flat : 2 * flat, :] = x_lo
    tile = 256

    def forward(j, carry):
        at = pl.ds(pl.multiple_of(j * tile, tile), tile)
        both = dot(wide[: 2 * flat, :], wave_hi[:, at])
        spec[:, at] = both[:flat] + both[flat:] + dot(wide[:flat, :], wave_lo[:, at])
        return carry

    lax.fori_loop(0, cols // tile, forward, 0)

    def pieces(hop):
        source = pl.ds((slab + n - hop) % n * slices, slices)
        steps = []
        for stage, (q, peer) in enumerate(((me, across), (me, mate), (across, mate))):
            for kind, buf in enumerate((band, halo)):
                ref = buf.at[0, q, source]
                at = (kind, stage, hop - 1)
                steps.append(remote(ref, ref, gs.at[at], gr.at[at], ang=peer))
        return steps

    passing = {}

    def pass_on(hop):
        first[2 * hop - 2].wait_recv()
        first[2 * hop - 1].wait_recv()
        passing[hop] = pieces(hop)
        for copy in passing[hop][:4]:
            copy.start()

    pass_on(1)

    for depth, target in ((rows, db), (HALO, dh)):
        row = lax.broadcasted_iota(jnp.int32, (rows, nz * depth), 0)
        col = lax.broadcasted_iota(jnp.int32, (rows, nz * depth), 1)
        for a in range(angles):
            moved = row - col % depth
            for z in range(nz):
                moved = jnp.where(col // depth == z, moved - off[a, z], moved)
            if target is dh:
                moved = moved + HALO
                hit = jnp.where(moved == 0, jnp.where(slab > 0, 1.0, 0.0), 0.0)
            else:
                hit = jnp.where(moved == 0, 1.0, 0.0)
            target[a * rows : (a + 1) * rows, :] = hit.astype(BF16)

    tall_rows = rows + HALO
    row = lax.broadcasted_iota(jnp.int32, (rows, 2 * angles * tall_rows), 0)
    col = lax.broadcasted_iota(jnp.int32, (rows, 2 * angles * tall_rows), 1)
    for z in range(nz):
        moved = col % tall_rows - row
        for a in range(angles):
            moved = jnp.where(col // tall_rows % angles == a, moved - off[a, z], moved)
        ub[z * rows : (z + 1) * rows, :] = jnp.where(moved == 0, 1.0, 0.0).astype(BF16)

    column = lax.broadcasted_iota(jnp.int32, (1, half), 1)
    base = column == 0
    omega = column.astype(F32) * (2.0 * math.pi / cols)
    turn_rate = jnp.where(base, math.pi, omega)
    weight = jnp.where(base, 1.0 / cols, 2.0 / cols)
    for a in range(angles):
        phase = turn_rate * shifts[a]
        cn, sn = jnp.cos(phase), jnp.sin(phase)
        cr = jnp.where(base, 1.0, cn)
        sr_ = jnp.where(base, 0.0, sn)
        re = spec[a * rows : (a + 1) * rows, :half]
        im = spec[a * rows : (a + 1) * rows, half:]
        parts = (
            (re * cr - im * sr_) * weight,
            (im * cn + re * sr_) * weight,
            (im * cr + re * sr_) * (-omega * weight),
            re * (omega * weight * cr) - im * (turn_rate * weight * sn),
        )
        for which in range(2):
            at = (which * angles + a) * rows
            for side in range(2):
                hi, lo = split(parts[2 * which + side])
                wide[at : at + rows, side * half : (side + 1) * half] = hi
                wide[2 * flat + at : 2 * flat + at + rows, side * half : (side + 1) * half] = lo

    for hop in range(2, n):
        pass_on(hop)

    def backward(j, carry):
        at = pl.ds(pl.multiple_of(j * tile, tile), tile)
        both = dot_t(wide[...], wave_hi[at, :])
        field[:, at] = both[: 2 * flat] + both[2 * flat :] + dot_t(wide[: 2 * flat, :], wave_lo[at, :])
        return carry

    lax.fori_loop(0, cols // tile, backward, 0)

    pending = list(first)
    for copy in local:
        copy.wait()
    for hop in range(1, n):
        for copy in passing[hop][:2]:
            copy.wait_recv()
        for copy in passing[hop][4:]:
            copy.start()
        pending.extend(passing[hop])
    zero_halo = jnp.zeros((nz, HALO, qc), BF16)
    for t in range(1, ROUNDS):
        halo[t, me] = zero_halo
        halo[t, across] = zero_halo
    w_copy.wait()

    def project(t, q, fresh_sum):
        moved = dot(db[...], band[t, q].reshape(nz * rows, qc)) + dot(dh[...], halo[t, q].reshape(nz * HALO, qc))
        hi, lo = split(moved)
        for a in range(angles):
            both = jnp.concatenate([hi[a * rows : (a + 1) * rows], lo[a * rows : (a + 1) * rows]], axis=0)
            part = dot(both, w[a, quarter(q), :])
            acc[a] = part if fresh_sum else acc[a] + part

    def spread(q, store):
        backs = [split(dot_t(ext_now[a], w[a, quarter(q), :])) for a in range(angles)]
        tall = jnp.concatenate([hi for hi, _ in backs] + [lo for _, lo in backs], axis=0)
        store(dot(ub[...], tall).astype(BF16).reshape(nz, rows, qc))

    upper = pl.ds(0, rows - HALO)
    lower = pl.ds(rows - HALO, HALO)
    for t in range(ROUNDS):
        last = t == ROUNDS - 1
        if t == 0:
            project(t, me, True)
            for hop in range(1, n):
                for copy in passing[hop][2:4]:
                    copy.wait_recv()
            project(t, mate, False)
            project(t, across, False)
            for hop in range(1, n):
                for copy in passing[hop][4:]:
                    copy.wait_recv()
            project(t, diagonal, False)
        else:
            shares[0].wait_recv()
            shares[2].wait_recv()
            project(t, mate, False)
            project(t, across, False)
            shares[1].wait_recv()
            shares[3].wait_recv()
            project(t, diagonal, False)
        ext_now = ext.at[t]
        for a in range(angles):
            projection = acc[a, :rows, :] + acc[a, rows:, :]
            residual = projection - field[a * rows : (a + 1) * rows, :]
            ext_now[a, :rows, :] = residual.astype(BF16)
            if last:
                res_out[a] = residual
                slope = field[(angles + a) * rows : (angles + a + 1) * rows, :]
                line = jnp.sum(projection * slope, axis=0, keepdims=True)
                sl[0, pl.ds(a, 1), :] = line
        edge = remote(ext_now.at[:, :HALO, :], ext_now.at[:, pl.ds(rows, HALO), :], rhs.at[t], rhr.at[t], slab=earlier)

        @pl.when(slab > 0)
        def _():
            edge.start()

        if last:
            slopes = []
            for hop in range(1, n):
                slopes.append(remote(sl.at[0], sl.at[hop], ss.at[hop - 1], sr.at[hop - 1], slab=(slab + hop) % n))
                slopes[-1].start()

        @pl.when(slab < n - 1)
        def _():
            edge.wait_recv()

        @pl.when(slab == n - 1)
        def _():
            ext_now[:, rows:, :] = jnp.zeros((angles, HALO, cols), BF16)

        def put(ref):
            def store(value):
                ref[...] = value
            return store

        sends = [
            remote(psend.at[t, slot], precv.at[t, slot], ps.at[t, slot], pr.at[t, slot], ang=mate)
            for slot in range(2)
        ]
        pending.extend(sends)

        def x_copy(half_, part, rows_):
            at = (t, 2 * half_ + part)
            return remote(xsend.at[t, half_, :, rows_, :], xrecv.at[t, half_, :, rows_, :], xs.at[at], xr.at[at], ang=across)

        spread(diagonal, put(psend.at[t, 0]))
        sends[0].start()
        spread(across, put(own))
        sends[0].wait_recv()
        xsend[t, 0] = (own[...].astype(F32) + precv[t, 0].astype(F32)).astype(BF16)
        if last:
            chunks = []
            for hop in list(range(1, n)) + [0]:
                to = pl.ds((slab + hop) % n * slices, slices)
                chunks.append((hop, to, remote(xsend.at[t, 0, to], xrecv.at[t, 0, to], cs.at[hop], cr_.at[hop], ang=across)))
                chunks[-1][2].start()
                pending.append(chunks[-1][2])
        else:
            x_copies = [x_copy(0, 0, lower), x_copy(0, 1, upper)]
            x_copies[0].start()
            x_copies[1].start()
        spread(mate, put(psend.at[t, 1]))
        sends[1].start()
        spread(me, put(own))
        sends[1].wait_recv()
        if not last:
            xsend[t, 1] = (own[...].astype(F32) + precv[t, 1].astype(F32)).astype(BF16)
            x_copies += [x_copy(1, 0, lower), x_copy(1, 1, upper)]
            x_copies[2].start()
            x_copies[3].start()
            pending.extend(x_copies)
            shares = []
            halos = []
            for k, q in enumerate((me, across)):
                ref = band.at[t + 1, q]
                shares.append(remote(ref, ref, ags.at[t, k], agr.at[t, k], ang=mate))
                halos.append(remote(band.at[t + 1, q, :, lower, :], halo.at[t + 1, q], hs.at[t, k], hr.at[t, k], slab=later))
            for k, q in enumerate((me, across)):
                ref = halo.at[t + 1, q]
                shares.append(remote(ref, ref, ags.at[t, 2 + k], agr.at[t, 2 + k], ang=mate))
            pending.extend(shares)

            def renew(k, q, rows_):
                gradient = xsend[t, 1 - k, :, rows_, :].astype(F32) + xrecv[t, k, :, rows_, :].astype(F32)
                kept = band[t, q, :, rows_, :].astype(F32)
                band[t + 1, q, :, rows_, :] = (kept - step_size * gradient).astype(BF16)

            def halo_start(k):
                @pl.when(slab < n - 1)
                def _():
                    halos[k].start()

            def halo_take(k):
                @pl.when(slab > 0)
                def _():
                    halos[k].wait_recv()

                shares[2 + k].start()

            x_copies[0].wait_recv()
            renew(0, me, lower)
            halo_start(0)
            x_copies[1].wait_recv()
            renew(0, me, upper)
            shares[0].start()
            x_copies[2].wait_recv()
            renew(1, across, lower)
            halo_start(1)
            halo_take(0)
            project(t + 1, me, True)
            x_copies[3].wait_recv()
            renew(1, across, upper)
            shares[1].start()
            halo_take(1)

            @pl.when(slab < n - 1)
            def _():
                halos[0].wait_send()
                halos[1].wait_send()

        @pl.when(slab > 0)
        def _():
            edge.wait_send()

    def out_steps(hop):
        e = (slab + n - hop) % n
        steps = []
        for stage, (q, peer) in enumerate(((me, across), (me, mate), (across, mate))):
            ref = out.at[:, band_rows(e), quarter(q)]
            steps.append(remote(ref, ref, os_.at[stage, hop], or_.at[stage, hop], ang=peer))
        return steps

    finals = []
    t = ROUNDS - 1
    for hop, to, chunk in chunks:
        chunk.wait_recv()
        gradient = own[to].astype(F32) + precv[t, 1, to].astype(F32) + xrecv[t, 0, to].astype(F32)
        renewed = (band[t, me, to].astype(F32) - step_size * gradient).astype(BF16)
        if hop:
            fresh[to] = renewed
            finals.append(remote(fresh.at[to], out.at[:, band_rows(slab), quarter(me)],
                                 fs.at[hop - 1], fr.at[hop - 1], slab=(slab + hop) % n))
            finals[-1].start()
        else:
            out[:, band_rows(slab), quarter(me)] = renewed
    ends = [out_steps(hop) for hop in range(n)]
    ends[0][0].start()
    ends[0][1].start()
    for copy in slopes:
        copy.wait_recv()
    total = sl[0]
    for hop in range(1, n):
        total = total + sl[hop]
    slope_out[...] = jnp.broadcast_to(
        jnp.sum(total, axis=1, keepdims=True) * (1.0 / math.sqrt(rows * n * cols)), slope_out.shape
    )
    for hop in range(1, n):
        finals[hop - 1].wait_recv()
        ends[hop][0].start()
        ends[hop][1].start()
    for steps in ends:
        steps[0].wait_recv()
        steps[2].start()
    for steps in ends:
        steps[1].wait_recv()
        steps[2].wait_recv()
        pending.extend(steps)
    for copy in pending + slopes + finals:
        copy.wait_send()


def fused(n, m, volume, ray_weights, row_offsets, measured, shifts):
    angles, rows, cols = measured.shape
    slices, _, xcells = volume.shape
    nz = slices * n
    qc = xcells // m
    flat = angles * rows
    quad = (nz, rows, qc)
    dma = pltpu.SemaphoreType.DMA
    vmem = pl.BlockSpec(memory_space=pltpu.VMEM)
    smem = pl.BlockSpec(memory_space=pltpu.SMEM)
    current, residual, slope = pl.pallas_call(
        functools.partial(fit_kernel, n, m),
        name="fit",
        out_shape=(
            jax.ShapeDtypeStruct(volume.shape, BF16),
            jax.ShapeDtypeStruct(measured.shape, F32),
            jax.ShapeDtypeStruct((angles, 128), F32),
        ),
        in_specs=[smem, smem, vmem, pl.BlockSpec(memory_space=pl.ANY), vmem] + [vmem] * 4,
        out_specs=(vmem, vmem, vmem),
        scratch_shapes=[
            pltpu.VMEM(ray_weights.shape, BF16),
            pltpu.VMEM((cols, cols), BF16),
            pltpu.VMEM((cols, cols), BF16),
            pltpu.VMEM((flat, cols), F32),
            pltpu.VMEM((4 * flat, cols), BF16),
            pltpu.VMEM((2 * flat, cols), F32),
            pltpu.VMEM((flat, nz * rows), BF16),
            pltpu.VMEM((flat, nz * HALO), BF16),
            pltpu.VMEM((nz * rows, 2 * angles * (rows + HALO)), BF16),
            pltpu.VMEM((ROUNDS, m) + quad, BF16),
            pltpu.VMEM((ROUNDS, m, nz, HALO, qc), BF16),
            pltpu.VMEM((angles, 2 * rows, cols), F32),
            pltpu.VMEM((ROUNDS, angles, rows + HALO, cols), BF16),
            pltpu.VMEM((ROUNDS, 2) + quad, BF16),
            pltpu.VMEM((ROUNDS, 2) + quad, BF16),
            pltpu.VMEM(quad, BF16),
            pltpu.VMEM((ROUNDS, 2) + quad, BF16),
            pltpu.VMEM((ROUNDS, 2) + quad, BF16),
            pltpu.VMEM(quad, BF16),
            pltpu.VMEM((n, angles, cols), F32),
            dma, dma((2 * m,)),
            dma((2 * n - 2,)), dma((2 * n - 2,)),
            dma((2, 3, n - 1)), dma((2, 3, n - 1)),
            dma((ROUNDS, 4)), dma((ROUNDS, 4)),
            dma((ROUNDS,)), dma((ROUNDS,)),
            dma((ROUNDS, 2)), dma((ROUNDS, 2)),
            dma((ROUNDS, 4)), dma((ROUNDS, 4)),
            dma((n,)), dma((n,)),
            dma((ROUNDS, 2)), dma((ROUNDS, 2)),
            dma((n - 1,)), dma((n - 1,)),
            dma((3, n)), dma((3, n)),
            dma((n - 1,)), dma((n - 1,)),
        ],
        compiler_params=pltpu.CompilerParams(
            collective_id=0, has_side_effects=True, vmem_limit_bytes=60 * 1024 * 1024
        ),
    )(row_offsets, shifts, volume, ray_weights, measured, *wave_tables(cols))
    return current, residual, slope[:, 0]


def step(n, m, volume, ray_weights, row_offsets, measured, shifts):
    band_rows = measured.shape[1]
    if m == 4 and n > 1 and band_rows % HALO == 0 and OFF <= HALO:
        return fused(n, m, volume, ray_weights, row_offsets, measured, shifts)
    return per_device(volume, ray_weights, row_offsets, measured, shifts)


def solution(mesh):
    local = functools.partial(step, mesh.shape["slab"], mesh.shape["ang"])
    in_specs = (
        P(("grp", "slab"), None, None),
        P("ang", None, None),
        P("ang", None),
        P(("grp", "ang"), "slab", None),
        P(("grp", "ang")),
    )
    out_specs = (P(("grp", "slab"), None, None), P(("grp", "ang"), "slab", None), P(("grp", "ang")))
    return jax.shard_map(
        local, mesh=mesh, in_specs=in_specs, out_specs=out_specs, check_vma=False
    )
```

```python
import math

import functools

import jax
import jax.numpy as jnp
import numpy as np
from jax import lax
from jax.experimental import pallas as pl
from jax.experimental.pallas import tpu as pltpu
from jax.sharding import PartitionSpec as P

Y = 256
X = 1024
U = 1024
OFF = 8
ROUNDS = 2


step_size = 0.5


def move_down(products, tilt_table):
    base = jnp.zeros((products.shape[1] + OFF, U), jnp.float32)
    placed = jax.vmap(
        lambda block, shift_rows: lax.dynamic_update_slice(base, block, (shift_rows, jnp.int32(0)))
    )(products, tilt_table)
    return jnp.sum(placed, axis=0)


def backproject(extended, tilt_table, ray_weights, band_rows):
    slices_count = tilt_table.shape[1]
    running = jnp.zeros((slices_count * band_rows, X), jnp.float32)
    for angle_index in range(ray_weights.shape[0]):
        source = extended[angle_index]
        picked = jax.vmap(
            lambda shift_rows: lax.dynamic_slice(source, (shift_rows, jnp.int32(0)), (band_rows, U))
        )(tilt_table[angle_index])
        running = running + lax.dot_general(
            picked.reshape(slices_count * band_rows, U),
            ray_weights[angle_index],
            (((1,), (1,)), ((), ())),
            preferred_element_type=jnp.float32,
        )
    return running


def apply_update(current, running):
    partial_value = lax.optimization_barrier(running.reshape(current.shape).astype(jnp.bfloat16))
    partial_wide = partial_value.astype(jnp.float32)
    gradient = lax.psum(partial_wide, "ang")
    renewed = (current.astype(jnp.float32) - step_size * gradient).astype(jnp.bfloat16)
    return renewed


def per_device(volume, ray_weights, row_offsets, measured, shifts):
    angles_here = ray_weights.shape[0]
    band_rows = measured.shape[1]
    highest = lax.Precision.HIGHEST
    numbers = lax.iota(jnp.int32, U)
    turns = numbers[:, None] * numbers[None, :] % U
    radians = turns.astype(jnp.float32) * (2.0 * math.pi / U)
    cosine = jnp.cos(radians)
    sine = jnp.sin(radians)
    signed = jnp.where(numbers <= (U - 1) // 2, numbers, numbers - U)
    omega = signed.astype(jnp.float32) * (2.0 * math.pi / U)
    flat_rows = measured.reshape(angles_here * band_rows, U)
    real_part = jnp.dot(flat_rows, cosine, precision=highest).reshape(angles_here, band_rows, U)
    imag_part = -jnp.dot(flat_rows, sine, precision=highest).reshape(angles_here, band_rows, U)
    phase = omega[None, None, :] * shifts[:, None, None]
    turned_real = real_part * jnp.cos(phase) + imag_part * jnp.sin(phase)
    turned_imag = imag_part * jnp.cos(phase) - real_part * jnp.sin(phase)
    first_half = jnp.concatenate([turned_real, omega * turned_imag], axis=0).reshape(-1, U)
    second_half = jnp.concatenate([turned_imag, -omega * turned_real], axis=0).reshape(-1, U)
    inverse = (
        jnp.dot(first_half, cosine, precision=highest)
        - jnp.dot(second_half, sine, precision=highest)
    ) / U
    inverse = inverse.reshape(2, angles_here, band_rows, U)
    shifted = inverse[0]
    slope_field = inverse[1]
    projection = shifted
    residual = shifted
    current = volume
    slices_here = volume.shape[0]
    tilt_table = lax.dynamic_slice_in_dim(
        row_offsets, lax.axis_index("slab") * slices_here, slices_here, 1
    )
    for round_index in range(ROUNDS):
        flattened = current.reshape(slices_here * Y, X)
        partials = jnp.stack(
            [
                move_down(
                    jnp.dot(
                        flattened, ray_weights[angle_index], preferred_element_type=jnp.float32
                    ).reshape(slices_here, Y, U),
                    tilt_table[angle_index],
                )[:Y]
                for angle_index in range(angles_here)
            ]
        )
        projection = lax.psum_scatter(partials, "slab", scatter_dimension=1, tiled=True)
        residual = projection - shifted
        rounded = residual.astype(jnp.bfloat16)
        gathered = lax.all_gather(rounded, "slab", axis=1, tiled=True)
        extended = jnp.concatenate(
            [gathered, jnp.zeros((angles_here, OFF, U), jnp.bfloat16)], axis=1
        )
        running = backproject(extended, tilt_table, ray_weights, Y)
        current = apply_update(current, running)
    local_dot = jnp.sum(projection * slope_field, axis=(1, 2))
    shift_slope = lax.psum(local_dot, "slab") / math.sqrt(Y * U)
    return (current, residual, shift_slope)


F32 = jnp.float32
BF16 = jnp.bfloat16
HALO = 16
FINE = 32


def wave_tables(columns):
    half = columns // 2
    k = np.arange(half)[None, :]
    coarse = np.arange(columns // FINE)[:, None] * FINE
    fine = np.arange(FINE)[:, None]
    turn = 2.0 * np.pi / columns
    coarse_turns = (coarse * k % columns) * turn
    fine_turns = (fine * k % columns) * turn
    fine_sine = np.sin(fine_turns)
    fine_sine[:, 0] = 1.0 - 2.0 * (np.arange(FINE) % 2)
    tables = (np.cos(coarse_turns), np.sin(coarse_turns), np.cos(fine_turns), fine_sine)
    return [jnp.asarray(t.astype(np.float32)) for t in tables]


def split(value):
    high = value.astype(BF16)
    return high, (value - high.astype(F32)).astype(BF16)


def dot(a, b):
    return jnp.dot(a, b, preferred_element_type=F32)


def dot_t(a, b):
    return lax.dot_general(a, b, (((1,), (1,)), ((), ())), preferred_element_type=F32)


def fit_kernel(
    n, m, off, shifts, vol, w_hbm, meas, ctab, stab, ftab, gtab,
    out, res_out, slope_out,
    w, wave_hi, wave_lo, spec, wide, field, db, dh, ub, band, halo, acc, ext,
    psend, precv, own, xsend, xrecv, fresh, sl,
    w_sem, loc_sem, zs, zr, gs, gr, ags, agr, rhs, rhr, ps, pr, xs, xr, cs, cr_, hs, hr, fs, fr, os_, or_, ss, sr,
):
    slab = lax.axis_index("slab")
    me = lax.axis_index("ang")
    angles, rows, cols = meas.shape
    slices = vol.shape[0]
    nz = slices * n
    qc = vol.shape[2] // m
    mate = me + 1 - 2 * (me % 2)
    across = (me + 2) % m
    diagonal = (mate + 2) % m
    later = (slab + 1) % n
    earlier = (slab + n - 1) % n

    def remote(src, dst, send, recv, **where):
        return pltpu.make_async_remote_copy(
            src_ref=src, dst_ref=dst, send_sem=send, recv_sem=recv,
            device_id=where, device_id_type=pl.DeviceIdType.MESH,
        )

    w_copy = pltpu.make_async_copy(w_hbm, w, w_sem)
    w_copy.start()
    barrier = pltpu.get_barrier_semaphore()
    for hop in range(1, n):
        pl.semaphore_signal(
            barrier, 1, device_id={"slab": (slab + hop) % n}, device_id_type=pl.DeviceIdType.MESH
        )
    for peer in (mate, across):
        pl.semaphore_signal(barrier, 1, device_id={"ang": peer}, device_id_type=pl.DeviceIdType.MESH)
    pl.semaphore_wait(barrier, n + 1)

    def quarter(q):
        return pl.ds(pl.multiple_of(q * qc, qc), qc)

    def band_rows(d):
        return pl.ds(pl.multiple_of(d * rows, rows), rows)

    def halo_rows(d):
        return pl.ds(pl.multiple_of((d + n - 1) % n * rows + rows - HALO, HALO), HALO)

    mine = pl.ds(slab * slices, slices)
    first = []
    for hop in range(1, n):
        d = (slab + hop) % n
        first.append(remote(vol.at[:, band_rows(d), quarter(me)], band.at[0, me, mine],
                            zs.at[hop - 1], zr.at[hop - 1], slab=d))
        first.append(remote(vol.at[:, halo_rows(d), quarter(me)], halo.at[0, me, mine],
                            zs.at[n - 2 + hop], zr.at[n - 2 + hop], slab=d))
    for copy in first:
        copy.start()
    local = []
    for q in range(m):
        columns = pl.ds(q * qc, qc)
        local.append(pltpu.make_async_copy(vol.at[:, band_rows(slab), columns], band.at[0, q, mine], loc_sem.at[2 * q]))
        local.append(pltpu.make_async_copy(vol.at[:, halo_rows(slab), columns], halo.at[0, q, mine], loc_sem.at[2 * q + 1]))
    for copy in local:
        copy.start()

    half = cols // 2

    def wave_rows(i, carry):
        at = pl.ds(pl.multiple_of(i * FINE, FINE), FINE)
        cc, cs = ctab[pl.ds(i, 1), :], stab[pl.ds(i, 1), :]
        fc, fs_ = ftab[...], gtab[...]
        hi, lo = split(cc * fc - cs * fs_)
        wave_hi[at, :half] = hi
        wave_lo[at, :half] = lo
        hi, lo = split(cs * fc + cc * fs_)
        wave_hi[at, half:] = hi
        wave_lo[at, half:] = lo
        return carry

    lax.fori_loop(0, cols // FINE, wave_rows, 0)
    flat = angles * rows
    x_hi, x_lo = split(meas[...].reshape(flat, cols))
    wide[:flat, :] = x_hi
    wide[flat : 2 * flat, :] = x_lo
    tile = 256

    def forward(j, carry):
        at = pl.ds(pl.multiple_of(j * tile, tile), tile)
        both = dot(wide[: 2 * flat, :], wave_hi[:, at])
        spec[:, at] = both[:flat] + both[flat:] + dot(wide[:flat, :], wave_lo[:, at])
        return carry

    lax.fori_loop(0, cols // tile, forward, 0)

    def pieces(hop):
        source = pl.ds((slab + n - hop) % n * slices, slices)
        steps = []
        for stage, (q, peer) in enumerate(((me, across), (me, mate), (across, mate))):
            for kind, buf in enumerate((band, halo)):
                ref = buf.at[0, q, source]
                at = (kind, stage, hop - 1)
                steps.append(remote(ref, ref, gs.at[at], gr.at[at], ang=peer))
        return steps

    passing = {}

    def pass_on(hop):
        first[2 * hop - 2].wait_recv()
        first[2 * hop - 1].wait_recv()
        passing[hop] = pieces(hop)
        for copy in passing[hop][:4]:
            copy.start()

    pass_on(1)

    for depth, target in ((rows, db), (HALO, dh)):
        row = lax.broadcasted_iota(jnp.int32, (rows, nz * depth), 0)
        col = lax.broadcasted_iota(jnp.int32, (rows, nz * depth), 1)
        for a in range(angles):
            moved = row - col % depth
            for z in range(nz):
                moved = jnp.where(col // depth == z, moved - off[a, z], moved)
            if target is dh:
                moved = moved + HALO
                hit = jnp.where(moved == 0, jnp.where(slab > 0, 1.0, 0.0), 0.0)
            else:
                hit = jnp.where(moved == 0, 1.0, 0.0)
            target[a * rows : (a + 1) * rows, :] = hit.astype(BF16)

    tall_rows = rows + HALO
    row = lax.broadcasted_iota(jnp.int32, (rows, 2 * angles * tall_rows), 0)
    col = lax.broadcasted_iota(jnp.int32, (rows, 2 * angles * tall_rows), 1)
    for z in range(nz):
        moved = col % tall_rows - row
        for a in range(angles):
            moved = jnp.where(col // tall_rows % angles == a, moved - off[a, z], moved)
        ub[z * rows : (z + 1) * rows, :] = jnp.where(moved == 0, 1.0, 0.0).astype(BF16)

    column = lax.broadcasted_iota(jnp.int32, (1, half), 1)
    base = column == 0
    omega = column.astype(F32) * (2.0 * math.pi / cols)
    turn_rate = jnp.where(base, math.pi, omega)
    weight = jnp.where(base, 1.0 / cols, 2.0 / cols)
    for a in range(angles):
        phase = turn_rate * shifts[a]
        cn, sn = jnp.cos(phase), jnp.sin(phase)
        cr = jnp.where(base, 1.0, cn)
        sr_ = jnp.where(base, 0.0, sn)
        re = spec[a * rows : (a + 1) * rows, :half]
        im = spec[a * rows : (a + 1) * rows, half:]
        parts = (
            (re * cr - im * sr_) * weight,
            (im * cn + re * sr_) * weight,
            (im * cr + re * sr_) * (-omega * weight),
            re * (omega * weight * cr) - im * (turn_rate * weight * sn),
        )
        for which in range(2):
            at = (which * angles + a) * rows
            for side in range(2):
                hi, lo = split(parts[2 * which + side])
                wide[at : at + rows, side * half : (side + 1) * half] = hi
                wide[2 * flat + at : 2 * flat + at + rows, side * half : (side + 1) * half] = lo

    for hop in range(2, n):
        pass_on(hop)

    def backward(j, carry):
        at = pl.ds(pl.multiple_of(j * tile, tile), tile)
        both = dot_t(wide[...], wave_hi[at, :])
        field[:, at] = both[: 2 * flat] + both[2 * flat :] + dot_t(wide[: 2 * flat, :], wave_lo[at, :])
        return carry

    lax.fori_loop(0, cols // tile, backward, 0)

    pending = list(first)
    for copy in local:
        copy.wait()
    for hop in range(1, n):
        for copy in passing[hop][:2]:
            copy.wait_recv()
        for copy in passing[hop][4:]:
            copy.start()
        pending.extend(passing[hop])
    zero_halo = jnp.zeros((nz, HALO, qc), BF16)
    for t in range(1, ROUNDS):
        halo[t, me] = zero_halo
        halo[t, across] = zero_halo
    w_copy.wait()

    def project(t, q, fresh_sum):
        moved = dot(db[...], band[t, q].reshape(nz * rows, qc)) + dot(dh[...], halo[t, q].reshape(nz * HALO, qc))
        hi, lo = split(moved)
        for a in range(angles):
            both = jnp.concatenate([hi[a * rows : (a + 1) * rows], lo[a * rows : (a + 1) * rows]], axis=0)
            part = dot(both, w[a, quarter(q), :])
            acc[a] = part if fresh_sum else acc[a] + part

    def spread(q, store):
        backs = [split(dot_t(ext_now[a], w[a, quarter(q), :])) for a in range(angles)]
        tall = jnp.concatenate([hi for hi, _ in backs] + [lo for _, lo in backs], axis=0)
        store(dot(ub[...], tall).astype(BF16).reshape(nz, rows, qc))

    upper = pl.ds(0, rows - HALO)
    lower = pl.ds(rows - HALO, HALO)
    for t in range(ROUNDS):
        last = t == ROUNDS - 1
        if t == 0:
            project(t, me, True)
            for hop in range(1, n):
                for copy in passing[hop][2:4]:
                    copy.wait_recv()
            project(t, mate, False)
            project(t, across, False)
            for hop in range(1, n):
                for copy in passing[hop][4:]:
                    copy.wait_recv()
            project(t, diagonal, False)
        else:
            shares[0].wait_recv()
            shares[2].wait_recv()
            project(t, mate, False)
            project(t, across, False)
            shares[1].wait_recv()
            shares[3].wait_recv()
            project(t, diagonal, False)
        ext_now = ext.at[t]
        for a in range(angles):
            projection = acc[a, :rows, :] + acc[a, rows:, :]
            residual = projection - field[a * rows : (a + 1) * rows, :]
            ext_now[a, :rows, :] = residual.astype(BF16)
            if last:
                res_out[a] = residual
                slope = field[(angles + a) * rows : (angles + a + 1) * rows, :]
                line = jnp.sum(projection * slope, axis=0, keepdims=True)
                sl[0, pl.ds(a, 1), :] = line
        edge = remote(ext_now.at[:, :HALO, :], ext_now.at[:, pl.ds(rows, HALO), :], rhs.at[t], rhr.at[t], slab=earlier)

        @pl.when(slab > 0)
        def _():
            edge.start()

        if last:
            slopes = []
            for hop in range(1, n):
                slopes.append(remote(sl.at[0], sl.at[hop], ss.at[hop - 1], sr.at[hop - 1], slab=(slab + hop) % n))
                slopes[-1].start()

        @pl.when(slab < n - 1)
        def _():
            edge.wait_recv()

        @pl.when(slab == n - 1)
        def _():
            ext_now[:, rows:, :] = jnp.zeros((angles, HALO, cols), BF16)

        def put(ref):
            def store(value):
                ref[...] = value
            return store

        sends = [
            remote(psend.at[t, slot], precv.at[t, slot], ps.at[t, slot], pr.at[t, slot], ang=mate)
            for slot in range(2)
        ]
        pending.extend(sends)

        def x_copy(half_, part, rows_):
            at = (t, 2 * half_ + part)
            return remote(xsend.at[t, half_, :, rows_, :], xrecv.at[t, half_, :, rows_, :], xs.at[at], xr.at[at], ang=across)

        spread(diagonal, put(psend.at[t, 0]))
        sends[0].start()
        spread(across, put(own))
        sends[0].wait_recv()
        xsend[t, 0] = (own[...].astype(F32) + precv[t, 0].astype(F32)).astype(BF16)
        if last:
            chunks = []
            for hop in list(range(1, n)) + [0]:
                to = pl.ds((slab + hop) % n * slices, slices)
                chunks.append((hop, to, remote(xsend.at[t, 0, to], xrecv.at[t, 0, to], cs.at[hop], cr_.at[hop], ang=across)))
                chunks[-1][2].start()
                pending.append(chunks[-1][2])
        else:
            x_copies = [x_copy(0, 0, lower), x_copy(0, 1, upper)]
            x_copies[0].start()
            x_copies[1].start()
        spread(mate, put(psend.at[t, 1]))
        sends[1].start()
        spread(me, put(own))
        sends[1].wait_recv()
        if not last:
            xsend[t, 1] = (own[...].astype(F32) + precv[t, 1].astype(F32)).astype(BF16)
            x_copies += [x_copy(1, 0, lower), x_copy(1, 1, upper)]
            x_copies[2].start()
            x_copies[3].start()
            pending.extend(x_copies)
            shares = []
            halos = []
            for k, q in enumerate((me, across)):
                ref = band.at[t + 1, q]
                shares.append(remote(ref, ref, ags.at[t, k], agr.at[t, k], ang=mate))
                halos.append(remote(band.at[t + 1, q, :, lower, :], halo.at[t + 1, q], hs.at[t, k], hr.at[t, k], slab=later))
            for k, q in enumerate((me, across)):
                ref = halo.at[t + 1, q]
                shares.append(remote(ref, ref, ags.at[t, 2 + k], agr.at[t, 2 + k], ang=mate))
            pending.extend(shares)

            def renew(k, q, rows_):
                gradient = xsend[t, 1 - k, :, rows_, :].astype(F32) + xrecv[t, k, :, rows_, :].astype(F32)
                kept = band[t, q, :, rows_, :].astype(F32)
                band[t + 1, q, :, rows_, :] = (kept - step_size * gradient).astype(BF16)

            def halo_start(k):
                @pl.when(slab < n - 1)
                def _():
                    halos[k].start()

            def halo_take(k):
                @pl.when(slab > 0)
                def _():
                    halos[k].wait_recv()

                shares[2 + k].start()

            x_copies[0].wait_recv()
            renew(0, me, lower)
            halo_start(0)
            x_copies[1].wait_recv()
            renew(0, me, upper)
            shares[0].start()
            x_copies[2].wait_recv()
            renew(1, across, lower)
            halo_start(1)
            halo_take(0)
            project(t + 1, me, True)
            x_copies[3].wait_recv()
            renew(1, across, upper)
            shares[1].start()
            halo_take(1)

            @pl.when(slab < n - 1)
            def _():
                halos[0].wait_send()
                halos[1].wait_send()

        @pl.when(slab > 0)
        def _():
            edge.wait_send()

    def out_steps(hop):
        e = (slab + n - hop) % n
        steps = []
        for stage, (q, peer) in enumerate(((me, across), (me, mate), (across, mate))):
            ref = out.at[:, band_rows(e), quarter(q)]
            steps.append(remote(ref, ref, os_.at[stage, hop], or_.at[stage, hop], ang=peer))
        return steps

    finals = []
    t = ROUNDS - 1
    for hop, to, chunk in chunks:
        chunk.wait_recv()
        gradient = own[to].astype(F32) + precv[t, 1, to].astype(F32) + xrecv[t, 0, to].astype(F32)
        renewed = (band[t, me, to].astype(F32) - step_size * gradient).astype(BF16)
        if hop:
            fresh[to] = renewed
            finals.append(remote(fresh.at[to], out.at[:, band_rows(slab), quarter(me)],
                                 fs.at[hop - 1], fr.at[hop - 1], slab=(slab + hop) % n))
            finals[-1].start()
        else:
            out[:, band_rows(slab), quarter(me)] = renewed
    ends = [out_steps(hop) for hop in range(n)]
    ends[0][0].start()
    ends[0][1].start()
    for copy in slopes:
        copy.wait_recv()
    total = sl[0]
    for hop in range(1, n):
        total = total + sl[hop]
    slope_out[...] = jnp.broadcast_to(
        jnp.sum(total, axis=1, keepdims=True) * (1.0 / math.sqrt(rows * n * cols)), slope_out.shape
    )
    for hop in range(1, n):
        finals[hop - 1].wait_recv()
        ends[hop][0].start()
        ends[hop][1].start()
    for steps in ends:
        steps[0].wait_recv()
        steps[2].start()
    for steps in ends:
        steps[1].wait_recv()
        steps[2].wait_recv()
        pending.extend(steps)
    for copy in pending + slopes + finals:
        copy.wait_send()


def place_kernel(current, residual, slope, current_out, residual_out, slope_out, sem_a, sem_b):
    copies = (
        pltpu.make_async_copy(current, current_out, sem_a),
        pltpu.make_async_copy(residual, residual_out, sem_b),
    )
    for copy in copies:
        copy.start()
    for a in range(slope.shape[0]):
        slope_out[a] = slope[a, 0]
    for copy in copies:
        copy.wait()


def fused(n, m, volume, ray_weights, row_offsets, measured, shifts):
    angles, rows, cols = measured.shape
    slices, _, xcells = volume.shape
    nz = slices * n
    qc = xcells // m
    flat = angles * rows
    quad = (nz, rows, qc)
    dma = pltpu.SemaphoreType.DMA
    vmem = pl.BlockSpec(memory_space=pltpu.VMEM)
    smem = pl.BlockSpec(memory_space=pltpu.SMEM)
    current, residual, slope = pl.pallas_call(
        functools.partial(fit_kernel, n, m),
        name="fit",
        out_shape=(
            jax.ShapeDtypeStruct(volume.shape, BF16),
            jax.ShapeDtypeStruct(measured.shape, F32),
            jax.ShapeDtypeStruct((angles, 128), F32),
        ),
        in_specs=[smem, smem, vmem, pl.BlockSpec(memory_space=pltpu.HBM), vmem] + [vmem] * 4,
        out_specs=(vmem, vmem, vmem),
        scratch_shapes=[
            pltpu.VMEM(ray_weights.shape, BF16),
            pltpu.VMEM((cols, cols), BF16),
            pltpu.VMEM((cols, cols), BF16),
            pltpu.VMEM((flat, cols), F32),
            pltpu.VMEM((4 * flat, cols), BF16),
            pltpu.VMEM((2 * flat, cols), F32),
            pltpu.VMEM((flat, nz * rows), BF16),
            pltpu.VMEM((flat, nz * HALO), BF16),
            pltpu.VMEM((nz * rows, 2 * angles * (rows + HALO)), BF16),
            pltpu.VMEM((ROUNDS, m) + quad, BF16),
            pltpu.VMEM((ROUNDS, m, nz, HALO, qc), BF16),
            pltpu.VMEM((angles, 2 * rows, cols), F32),
            pltpu.VMEM((ROUNDS, angles, rows + HALO, cols), BF16),
            pltpu.VMEM((ROUNDS, 2) + quad, BF16),
            pltpu.VMEM((ROUNDS, 2) + quad, BF16),
            pltpu.VMEM(quad, BF16),
            pltpu.VMEM((ROUNDS, 2) + quad, BF16),
            pltpu.VMEM((ROUNDS, 2) + quad, BF16),
            pltpu.VMEM(quad, BF16),
            pltpu.VMEM((n, angles, cols), F32),
            dma, dma((2 * m,)),
            dma((2 * n - 2,)), dma((2 * n - 2,)),
            dma((2, 3, n - 1)), dma((2, 3, n - 1)),
            dma((ROUNDS, 4)), dma((ROUNDS, 4)),
            dma((ROUNDS,)), dma((ROUNDS,)),
            dma((ROUNDS, 2)), dma((ROUNDS, 2)),
            dma((ROUNDS, 4)), dma((ROUNDS, 4)),
            dma((n,)), dma((n,)),
            dma((ROUNDS, 2)), dma((ROUNDS, 2)),
            dma((n - 1,)), dma((n - 1,)),
            dma((3, n)), dma((3, n)),
            dma((n - 1,)), dma((n - 1,)),
        ],
        compiler_params=pltpu.CompilerParams(
            collective_id=0, has_side_effects=True, vmem_limit_bytes=36 * 1024 * 1024
        ),
    )(row_offsets, shifts, volume, ray_weights, measured, *wave_tables(cols))
    hbm = pl.BlockSpec(memory_space=pl.ANY)
    return pl.pallas_call(
        place_kernel,
        name="place",
        out_shape=(
            jax.ShapeDtypeStruct(volume.shape, BF16),
            jax.ShapeDtypeStruct(measured.shape, F32),
            jax.ShapeDtypeStruct((angles,), F32),
        ),
        in_specs=[vmem, vmem, vmem],
        out_specs=(hbm, hbm, smem),
        scratch_shapes=[dma, dma],
        compiler_params=pltpu.CompilerParams(vmem_limit_bytes=8 * 1024 * 1024),
    )(current, residual, slope)


def step(n, m, volume, ray_weights, row_offsets, measured, shifts):
    band_rows = measured.shape[1]
    if m == 4 and n > 1 and band_rows % HALO == 0 and OFF <= HALO:
        return fused(n, m, volume, ray_weights, row_offsets, measured, shifts)
    return per_device(volume, ray_weights, row_offsets, measured, shifts)


def solution(mesh):
    local = functools.partial(step, mesh.shape["slab"], mesh.shape["ang"])
    in_specs = (
        P(("grp", "slab"), None, None),
        P("ang", None, None),
        P("ang", None),
        P(("grp", "ang"), "slab", None),
        P(("grp", "ang")),
    )
    out_specs = (P(("grp", "slab"), None, None), P(("grp", "ang"), "slab", None), P(("grp", "ang")))
    return jax.shard_map(
        local, mesh=mesh, in_specs=in_specs, out_specs=out_specs, check_vma=False
    )
```
